32 devices in a mesh: seq: 4 (over x, core), tp: 8 (over z, y).
Axes of the slice: x: 2, y: 2, z: 4, core: 2. Of those that a mesh axis runs over, the one named last changes fastest.
Arguments:
- vit_input: bfloat16 [2048, 1280], P(('seq', 'tp')), may hold values from -6 to 6
- image_lengths: int32 [4, 2], P('seq'), may hold values from 1 to 96, 128 in all within a row
- positions: int32 [512], replicated, may hold values from 0 to 511, each once
- vit_ln_gain: float32 [1280], replicated, may hold values from 0.25 to 1.75
- w_qkv: bfloat16 [1280, 3, 1280], P(None, None, 'tp'), may hold values from -0.15625 to 0.15625
- w_proj: bfloat16 [1280, 1280], P('tp'), may hold values from -0.15625 to 0.15625
- merger_ln_gain: float32 [1280], replicated, may hold values from 0.25 to 1.75
- merger_w1: bfloat16 [5120, 5120], P(None, 'tp'), may hold values from -0.078125 to 0.078125
- merger_w2: bfloat16 [5120, 8192], P('tp'), may hold values from -0.36336105 to 0.36336105
- norm_gain: float32 [8192], P('seq'), may hold values from 0.25 to 1.75
- gate_up_weight: bfloat16 [8192, 2, 29568], P('seq', None, 'tp'), may hold values from -0.0625 to 0.0625
- down_weight: bfloat16 [29568, 8192], P('tp', 'seq'), may hold values from -0.125 to 0.125
Outputs:
- mixed: bfloat16 [512, 8192], P('tp', 'seq')
The draws below stay inside these ranges and needn't reach their ends.
Inputs may be any that keep to these rules, and one draw needn't show every extreme that they name: `image_lengths`: each row sums to 128. `positions`: a permutation: every slot once.
All inputs are finite; a program needn't handle non-finite values.
Results may differ from the reference program's by a relative error of at most 0.038.
Values may be sent and summed in bfloat16 or wider, within the bound.
A program may use at most 128 MiB of HBM per device.

```python
import math
import jax
import jax.numpy as jnp
import numpy as np
from jax import lax

VW = 1280
HEADS = 16
D = 8192
FF = 29568
IMG_GROUP = 2
HD = 80
MW = 5120
GROUPS = 4
GROUP_TOK = 128
TOKENS = 512
PATCHES = 2048
N_SEQ = 4
N_TP = 8


def draw_merger_w2(key, part):
    first = jax.random.fold_in(key, 11)
    second = jax.random.fold_in(key, 23)
    third = jax.random.fold_in(key, 37)
    base = jnp.clip(jax.random.normal(first, (MW, D), jnp.float32), -6.0, 6.0)
    column_place = jnp.arange(D, dtype=jnp.float32) / D
    rough = jnp.exp(jax.random.uniform(second, (D,), jnp.float32, jnp.log(0.7), jnp.log(1.4)))
    column_scale = jnp.exp(jnp.log(3.0) * column_place) * rough
    pairing = jax.random.permutation(third, N_TP)
    row_block = jnp.arange(MW, dtype=jnp.int32) // (MW // N_TP)
    col_block = jnp.arange(D, dtype=jnp.int32) // (D // N_TP)
    spiked = pairing[row_block][:, None] == col_block[None, :]
    boost = jnp.where(spiked, 4.0, 1.0)
    values = base * boost * column_scale[None, :] / jnp.sqrt(16.0 * MW)
    return values.astype(jnp.bfloat16)


def levels(key, extent, shards, smallest, high):
    factor_of = 1.0
    for axis_at, blocks in shards:
        steps = jax.random.uniform(jax.random.fold_in(jax.random.fold_in(key, 6), axis_at), (blocks,), jnp.float32, smallest / len(shards), high / len(shards))
        factor_of = factor_of * jnp.repeat(jnp.exp(steps), extent[axis_at] // blocks).reshape((-1,) + (1,) * (len(extent) - 1 - axis_at))
    return factor_of


def length_profile(number_of, total, limit, slope):
    portions = [(1 << 20) // math.isqrt(standing ** slope) + 1 for standing in range(2, number_of + 1)]
    spare, holding = total - limit - (number_of - 1), [1] * (number_of - 1)
    while spare > 0:
        free = [i for i in range(number_of - 1) if holding[i] < limit]
        pool, remaining = sum([portions[i] for i in free]), spare
        for i in free:
            more = min(limit - holding[i], max(1, remaining * portions[i] // pool), spare)
            holding[i] = holding[i] + more
            spare = spare - more
    return np.array([limit] + holding)


def uneven(stream_key, number_of, total, limit, lean):
    if number_of == 2:
        one = jax.random.randint(stream_key, (), max(1, total - limit), min(limit, total - 1) + 1)
        return jnp.stack([one, total - one])
    tallies = jnp.asarray(length_profile(number_of, total, limit, lean), jnp.int32)
    twos = (number_of - 1) // 2
    source_of, receiver = tallies[1:1 + 2 * twos:2], tallies[2:2 + 2 * twos:2]
    slack = jnp.minimum(source_of - 1, limit - receiver)
    moved = jax.random.randint(jax.random.fold_in(stream_key, 1), (twos,), 0, 1 << 20) % (slack + 1)
    tallies = tallies.at[1:1 + 2 * twos:2].set(source_of - moved).at[2:2 + 2 * twos:2].set(receiver + moved)
    return tallies[jax.random.permutation(jax.random.fold_in(stream_key, 2), number_of)]


def bell_draw(rng, dims, scale, reach, pieces=(), kind=jnp.bfloat16):
    factor_of = levels(rng, dims, pieces, -0.22, 0.18) if pieces else 1.0
    entries = jax.random.normal(rng, dims, jnp.float32) * scale * factor_of
    return jnp.minimum(jnp.maximum(entries, -reach), reach).astype(kind)


def setup_inputs(seed: int = 0) -> dict:
    streams_of = jax.random.split(jax.random.key(seed), 13)
    return {
        "vit_input": bell_draw(streams_of[0], (PATCHES, VW), 1.0, 6.0, ((0, 32),)),
        "image_lengths": jax.vmap(lambda own: uneven(own, IMG_GROUP, GROUP_TOK, GROUP_TOK * 3 // 4, 2))(jax.random.split(streams_of[1], GROUPS)).reshape((GROUPS, IMG_GROUP)).astype(jnp.int32),
        "positions": jax.random.permutation(streams_of[2], TOKENS).astype(jnp.int32),
        "vit_ln_gain": jnp.clip(1.0 + 0.15 * jax.random.normal(streams_of[3], (VW,), jnp.float32), 0.25, 1.75),
        "w_qkv": bell_draw(streams_of[4], (VW, 3, VW), VW ** -0.5, 0.15625, ((2, 8),)),
        "w_proj": bell_draw(streams_of[5], (VW, VW), VW ** -0.5, 0.15625, ((0, 8),)),
        "merger_ln_gain": jnp.clip(1.0 + 0.15 * jax.random.normal(streams_of[6], (VW,), jnp.float32), 0.25, 1.75),
        "merger_w1": bell_draw(streams_of[7], (MW, MW), MW ** -0.5, 0.078125, ((1, 8),)),
        "merger_w2": draw_merger_w2(jax.random.fold_in(streams_of[12], 71), 0),
        "norm_gain": jnp.clip(1.0 + 0.15 * jax.random.normal(streams_of[9], (D,), jnp.float32), 0.25, 1.75),
        "gate_up_weight": bell_draw(streams_of[10], (D, 2, FF), D ** -0.5, 0.0625, ((0, 4), (2, 8))),
        "down_weight": bell_draw(streams_of[11], (FF, D), (FF // 16) ** -0.5, 0.125, ((0, 8), (1, 4))),
    }


def layer_norm(values, gain):
    mean = lax.optimization_barrier(jnp.mean(values, axis=-1, keepdims=True))
    centered = values - mean
    variance = lax.optimization_barrier(jnp.mean(centered * centered, axis=-1, keepdims=True))
    return centered * lax.rsqrt(variance + 1e-06) * gain

def image_ids(lengths, count):
    image_ends = jnp.cumsum(lengths.astype(jnp.int32)) * 4
    patch_index = jnp.arange(count, dtype=jnp.int32)
    return lax.optimization_barrier(jnp.sum((patch_index[:, None] >= image_ends[None, :]).astype(jnp.int32), axis=1))

def wire_round(values):
    return lax.optimization_barrier(values.astype(jnp.bfloat16)).astype(jnp.float32)

def attend(query, keys, values, image_index):
    scores = jnp.einsum('qhe,khe->hqk', query.astype(jnp.float32), keys.astype(jnp.float32)) * HD ** (-0.5)
    same_image = image_index[:, None] == image_index[None, :]
    scores = jnp.where(same_image[None], scores, -1e+30)
    top = lax.optimization_barrier(jnp.max(scores, axis=-1, keepdims=True))
    expo = jnp.exp(scores - top)
    weights = (expo / lax.optimization_barrier(jnp.sum(expo, axis=-1, keepdims=True))).astype(jnp.bfloat16)
    output = jnp.einsum('hqk,khe->qhe', weights.astype(jnp.float32), values.astype(jnp.float32))
    return output.astype(jnp.bfloat16)

def slot_sources(positions):
    count = positions.shape[0]
    return jnp.zeros((count,), jnp.int32).at[positions.astype(jnp.int32)].set(jnp.arange(count, dtype=jnp.int32))

def reference(vit_input, image_lengths, positions, vit_ln_gain, w_qkv, w_proj, merger_ln_gain, merger_w1, merger_w2, norm_gain, gate_up_weight, down_weight):
    group_patches = PATCHES // N_SEQ
    normed_patches = layer_norm(vit_input.astype(jnp.float32), vit_ln_gain).astype(jnp.bfloat16)
    projected = jnp.dot(normed_patches, w_qkv.reshape(VW, 3 * VW), preferred_element_type=jnp.float32).astype(jnp.bfloat16)
    projected = projected.reshape(N_SEQ, group_patches, 3, HEADS, HD)

    def per_group(pair):
        block, lengths = pair
        image_index = image_ids(lengths, group_patches)
        return attend(block[:, 0], block[:, 1], block[:, 2], image_index)
    attended = lax.map(per_group, (projected, image_lengths)).reshape(PATCHES, VW)
    head_cols = VW // N_TP
    attn_sum = jnp.zeros((PATCHES, VW), jnp.float32)
    for block_index in range(N_TP):
        lower = block_index * head_cols
        attn_sum = attn_sum + wire_round(jnp.dot(attended[:, lower:lower + head_cols], w_proj[lower:lower + head_cols], preferred_element_type=jnp.float32))
    vit_out = vit_input.astype(jnp.float32) + attn_sum
    merged_in = layer_norm(vit_out, merger_ln_gain).astype(jnp.bfloat16).reshape(TOKENS, MW)
    expanded = jax.nn.gelu(jnp.dot(merged_in, merger_w1, preferred_element_type=jnp.float32), approximate=False).astype(jnp.bfloat16)
    merge_cols = MW // N_TP
    vis_sum = jnp.zeros((TOKENS, D), jnp.float32)
    for block_index in range(N_TP):
        lower = block_index * merge_cols
        vis_sum = vis_sum + wire_round(jnp.dot(expanded[:, lower:lower + merge_cols], merger_w2[lower:lower + merge_cols], preferred_element_type=jnp.float32))
    vis = vis_sum.astype(jnp.bfloat16)
    seq_tokens = jnp.take(vis, slot_sources(positions), axis=0)
    token_values = seq_tokens.astype(jnp.float32)
    row_squares = lax.optimization_barrier(jnp.sum(token_values * token_values, axis=1))
    inverse_rms = lax.rsqrt(row_squares / D + 1e-06)
    normed = (token_values * inverse_rms[:, None] * norm_gain).astype(jnp.bfloat16)
    slice_width = D // N_SEQ
    gate_up = jnp.zeros((TOKENS, 2 * FF), jnp.float32)
    for block_index in range(N_SEQ):
        lower = block_index * slice_width
        weight_block = gate_up_weight[lower:lower + slice_width].reshape(slice_width, 2 * FF)
        gate_up = gate_up + wire_round(jnp.dot(normed[:, lower:lower + slice_width], weight_block, preferred_element_type=jnp.float32))
    hidden = (jax.nn.silu(gate_up[:, :FF]) * gate_up[:, FF:]).astype(jnp.bfloat16)
    hidden_cols = FF // N_TP
    down_sum = jnp.zeros((TOKENS, D), jnp.float32)
    for block_index in range(N_TP):
        lower = block_index * hidden_cols
        down_sum = down_sum + wire_round(jnp.dot(hidden[:, lower:lower + hidden_cols], down_weight[lower:lower + hidden_cols], preferred_element_type=jnp.float32))
    return (token_values + down_sum).astype(jnp.bfloat16)
```

```python
import functools

import jax
import jax.numpy as jnp
from jax import lax
from jax.experimental import pallas as pl
from jax.experimental.pallas import tpu as pltpu
from jax.sharding import PartitionSpec as P

D = 8192
HD = 80
MESH = pl.DeviceIdType.MESH
VM = pl.BlockSpec(memory_space=pltpu.VMEM)


def factors(n):
    minor = max(d for d in range(1, n + 1) if n % d == 0 and d * d <= n)
    return n // minor, minor


def greet(axis, peers):
    barrier = pltpu.get_barrier_semaphore()
    for peer in peers:
        pl.semaphore_signal(barrier, inc=1, device_id={axis: peer}, device_id_type=MESH)
    pl.semaphore_wait(barrier, len(peers))


def grid_peers(n_a, n_b, a, b):
    along_a = [lax.rem(a + da, n_a) * n_b + b for da in range(1, n_a)]
    along_b = [a * n_b + lax.rem(b + db, n_b) for db in range(1, n_b)]
    return along_a, along_b


def send(src, dst, send_sem, recv_sem, axis, peer):
    copy = pltpu.make_async_remote_copy(
        src_ref=src,
        dst_ref=dst,
        send_sem=send_sem,
        recv_sem=recv_sem,
        device_id={axis: peer},
        device_id_type=MESH,
    )
    copy.start()
    return copy


def gather_kernel(axis, n, x_ref, out_ref, a_send, a_recv, b_send, b_recv, own_sem):
    n_a, n_b = factors(n)
    me = lax.axis_index(axis)
    a, b = me // n_b, lax.rem(me, n_b)
    along_a, along_b = grid_peers(n_a, n_b, a, b)
    greet(axis, along_a + along_b)
    a_copies, b_copies = [None], []
    for da in range(1, n_a):
        a_copies.append(
            send(x_ref, out_ref.at[me], a_send.at[da - 1], a_recv.at[da - 1], axis, along_a[da - 1])
        )
    own = pltpu.make_async_copy(x_ref, out_ref.at[me], own_sem)
    own.start()
    for db in range(1, n_b):
        b_copies.append(
            send(x_ref, out_ref.at[me], b_send.at[0, db - 1], b_recv.at[0, db - 1], axis, along_b[db - 1])
        )
    order = sorted(range(1, n_a), key=lambda da: min(da, n_a - da))
    for da in order:
        a_copies[da].wait_recv()
        source = lax.rem(a - da + n_a, n_a) * n_b + b
        for db in range(1, n_b):
            b_copies.append(
                send(
                    out_ref.at[source],
                    out_ref.at[source],
                    b_send.at[da, db - 1],
                    b_recv.at[da, db - 1],
                    axis,
                    along_b[db - 1],
                )
            )
    for copy in b_copies:
        copy.wait()
    for copy in a_copies[1:]:
        copy.wait_send()
    own.wait()


def gather(x, axis, collective_id):
    n = lax.axis_size(axis)
    n_a, n_b = factors(n)
    dma = pltpu.SemaphoreType.DMA
    return pl.pallas_call(
        functools.partial(gather_kernel, axis, n),
        out_shape=jax.ShapeDtypeStruct((n,) + x.shape, x.dtype),
        in_specs=[VM],
        out_specs=VM,
        scratch_shapes=[
            dma((n_a,)),
            dma((n_a,)),
            dma((n_a, n_b)),
            dma((n_a, n_b)),
            dma,
        ],
        name=f"gather{collective_id}",
        compiler_params=pltpu.CompilerParams(collective_id=collective_id, has_side_effects=True),
    )(x)


def scatter_kernel(axis, n, x_ref, out_ref, r1, y, r2, a_send, a_recv, b_send, b_recv):
    n_a, n_b = factors(n)
    me = lax.axis_index(axis)
    a, b = me // n_b, lax.rem(me, n_b)
    along_a, along_b = grid_peers(n_a, n_b, a, b)
    greet(axis, along_a + along_b)
    order = sorted(range(1, n_a), key=lambda da: -min(da, n_a - da)) + [0]
    b_copies, a_copies = {}, []
    for da in order:
        for db in range(1, n_b):
            block = lax.rem(a + da, n_a) * n_b + lax.rem(b + db, n_b)
            b_copies[da, db] = send(
                x_ref.at[block],
                r1.at[da, db - 1],
                b_send.at[da, db - 1],
                b_recv.at[da, db - 1],
                axis,
                along_b[db - 1],
            )

    def arrived(da):
        total = x_ref[lax.rem(a + da, n_a) * n_b + b].astype(jnp.float32)
        for db in range(1, n_b):
            b_copies[da, db].wait_recv()
            total = total + r1[da, db - 1].astype(jnp.float32)
        return total

    for da in order[:-1]:
        y[da - 1] = arrived(da).astype(y.dtype)
        a_copies.append(
            send(y.at[da - 1], r2.at[da - 1], a_send.at[da - 1], a_recv.at[da - 1], axis, along_a[da - 1])
        )
    total = arrived(0)
    for da, copy in zip(order[:-1], a_copies):
        copy.wait_recv()
        total = total + r2[da - 1].astype(jnp.float32)
    out_ref[...] = total.astype(out_ref.dtype)
    for copy in b_copies.values():
        copy.wait_send()
    for copy in a_copies:
        copy.wait_send()


def scatter_sum(x, axis, dtype, collective_id):
    n = lax.axis_size(axis)
    n_a, n_b = factors(n)
    block = x.shape[1:]
    dma = pltpu.SemaphoreType.DMA
    return pl.pallas_call(
        functools.partial(scatter_kernel, axis, n),
        out_shape=jax.ShapeDtypeStruct(block, dtype),
        in_specs=[VM],
        out_specs=VM,
        scratch_shapes=[
            pltpu.VMEM((n_a, n_b - 1) + block, x.dtype),
            pltpu.VMEM((n_a - 1,) + block, x.dtype),
            pltpu.VMEM((n_a - 1,) + block, x.dtype),
            dma((n_a,)),
            dma((n_a,)),
            dma((n_a, n_b)),
            dma((n_a, n_b)),
        ],
        name=f"scatter_sum{collective_id}",
        compiler_params=pltpu.CompilerParams(collective_id=collective_id, has_side_effects=True),
    )(x)


def exchange_kernel(axis, n, x_ref, out_ref, send_sem, recv_sem, own_sem):
    me = lax.axis_index(axis)
    peers = [lax.rem(me + d, n) for d in range(1, n)]
    greet(axis, peers)
    copies = [
        send(x_ref.at[peer], out_ref.at[me], send_sem.at[i], recv_sem.at[i], axis, peer)
        for i, peer in enumerate(peers)
    ]
    own = pltpu.make_async_copy(x_ref.at[me], out_ref.at[me], own_sem)
    own.start()
    for copy in copies:
        copy.wait()
    own.wait()


def exchange(x, axis, collective_id):
    n = lax.axis_size(axis)
    dma = pltpu.SemaphoreType.DMA
    return pl.pallas_call(
        functools.partial(exchange_kernel, axis, n),
        out_shape=jax.ShapeDtypeStruct(x.shape, x.dtype),
        in_specs=[VM],
        out_specs=VM,
        scratch_shapes=[dma((n,)), dma((n,)), dma],
        name=f"exchange{collective_id}",
        compiler_params=pltpu.CompilerParams(collective_id=collective_id, has_side_effects=True),
    )(x)


def hidden_kernel(axis, n, gu_ref, h_ref, r1, y, r2, own_h, b_send, b_recv, a_send, a_recv, ga_send, ga_recv, gb_send, gb_recv, own_sem):
    n_a, n_b = factors(n)
    chunks = gu_ref.shape[0]
    width = gu_ref.shape[3] // n
    me = lax.axis_index(axis)
    a, b = me // n_b, lax.rem(me, n_b)
    along_a, along_b = grid_peers(n_a, n_b, a, b)

    def lanes(owner):
        return pl.ds(pl.multiple_of(owner * width, width), width)

    greet(axis, along_a + along_b)
    order = sorted(range(1, n_a), key=lambda da: -min(da, n_a - da)) + [0]
    b_copies, a_copies, ga, gb, local = {}, {}, {}, [], []
    for c in range(chunks):
        for da in order:
            for db in range(1, n_b):
                block = lax.rem(a + da, n_a) * n_b + lax.rem(b + db, n_b)
                b_copies[c, da, db] = send(
                    gu_ref.at[c, :, :, lanes(block)],
                    r1.at[c, da, db - 1],
                    b_send.at[c, da, db - 1],
                    b_recv.at[c, da, db - 1],
                    axis,
                    along_b[db - 1],
                )

    def arrived(c, da):
        block = lax.rem(a + da, n_a) * n_b + b
        total = gu_ref[c, :, :, lanes(block)].astype(jnp.float32)
        for db in range(1, n_b):
            b_copies[c, da, db].wait_recv()
            total = total + r1[c, da, db - 1].astype(jnp.float32)
        return total

    for c in range(chunks):
        for da in order[:-1]:
            y[c, da - 1] = arrived(c, da).astype(y.dtype)
            a_copies[c, da] = send(
                y.at[c, da - 1],
                r2.at[c, da - 1],
                a_send.at[c, da - 1],
                a_recv.at[c, da - 1],
                axis,
                along_a[da - 1],
            )

    def relay(c):
        for da in sorted(range(1, n_a), key=lambda da: min(da, n_a - da)):
            ga[c, da].wait_recv()
            source = h_ref.at[c, :, lanes(lax.rem(a - da + n_a, n_a) * n_b + b)]
            for db in range(1, n_b):
                gb.append(
                    send(source, source, gb_send.at[c, da, db - 1], gb_recv.at[c, da, db - 1], axis, along_b[db - 1])
                )

    for c in range(chunks):
        total = arrived(c, 0)
        for da in order[:-1]:
            a_copies[c, da].wait_recv()
            total = total + r2[c, da - 1].astype(jnp.float32)
        own_h[c] = (jax.nn.silu(total[0]) * total[1]).astype(own_h.dtype)
        target = h_ref.at[c, :, lanes(me)]
        for da in order[:-1]:
            ga[c, da] = send(own_h.at[c], target, ga_send.at[c, da - 1], ga_recv.at[c, da - 1], axis, along_a[da - 1])
        for db in range(1, n_b):
            gb.append(send(own_h.at[c], target, gb_send.at[c, 0, db - 1], gb_recv.at[c, 0, db - 1], axis, along_b[db - 1]))
        copy = pltpu.make_async_copy(own_h.at[c], target, own_sem.at[c])
        copy.start()
        local.append(copy)
    for c in range(chunks):
        relay(c)
    for copy in gb:
        copy.wait()
    for copy in list(b_copies.values()) + list(a_copies.values()) + list(ga.values()):
        copy.wait_send()
    for copy in local:
        copy.wait()


def hidden_values(gu, axis, collective_id):
    n = lax.axis_size(axis)
    n_a, n_b = factors(n)
    chunks, _, rows, tokens = gu.shape
    width = tokens // n
    dma = pltpu.SemaphoreType.DMA
    pair = (2, rows, width)
    return pl.pallas_call(
        functools.partial(hidden_kernel, axis, n),
        out_shape=jax.ShapeDtypeStruct((chunks, rows, tokens), gu.dtype),
        in_specs=[VM],
        out_specs=VM,
        scratch_shapes=[
            pltpu.VMEM((chunks, n_a, n_b - 1) + pair, gu.dtype),
            pltpu.VMEM((chunks, n_a - 1) + pair, gu.dtype),
            pltpu.VMEM((chunks, n_a - 1) + pair, gu.dtype),
            pltpu.VMEM((chunks, rows, width), gu.dtype),
            dma((chunks, n_a, n_b)),
            dma((chunks, n_a, n_b)),
            dma((chunks, n_a)),
            dma((chunks, n_a)),
            dma((chunks, n_a)),
            dma((chunks, n_a)),
            dma((chunks, n_a, n_b)),
            dma((chunks, n_a, n_b)),
            dma((chunks,)),
        ],
        name="hidden",
        compiler_params=pltpu.CompilerParams(
            collective_id=collective_id, has_side_effects=True, vmem_limit_bytes=67_000_000
        ),
    )(gu)


def chunk_count(rows):
    for count in (7, 6, 4, 3, 2):
        if rows % (count * 8) == 0:
            return count
    return 1


def layer_norm(values, gain):
    mean = jnp.mean(values, axis=-1, keepdims=True)
    centered = values - mean
    variance = jnp.mean(centered * centered, axis=-1, keepdims=True)
    return centered * lax.rsqrt(variance + 1e-06) * gain


def image_ids(lengths, count):
    image_ends = jnp.cumsum(lengths) * 4
    patch_index = jnp.arange(count, dtype=jnp.int32)
    return jnp.sum((patch_index[:, None] >= image_ends[None, :]).astype(jnp.int32), axis=1)


def attend(query, keys, values, image_index):
    scores = jnp.einsum("qhe,khe->hqk", query, keys, preferred_element_type=jnp.float32) * HD ** (
        -0.5
    )
    same_image = image_index[:, None] == image_index[None, :]
    scores = jnp.where(same_image[None], scores, -1e30)
    top = jnp.max(scores, axis=-1, keepdims=True)
    expo = jnp.exp(scores - top)
    weights = (expo / jnp.sum(expo, axis=-1, keepdims=True)).astype(jnp.bfloat16)
    output = jnp.einsum("hqk,khe->qhe", weights, values, preferred_element_type=jnp.float32)
    return output.astype(jnp.bfloat16)


def local(
    vit_input,
    image_lengths,
    positions,
    vit_ln_gain,
    w_qkv,
    w_proj,
    merger_ln_gain,
    merger_w1,
    merger_w2,
    norm_gain,
    gate_up_weight,
    down_weight,
):
    tp_size = lax.axis_size("tp")
    own_patches = vit_input.shape[0]
    patch_width = vit_input.shape[1]
    head_cols = w_qkv.shape[2]
    local_heads = head_cols // HD
    normed_patches = layer_norm(vit_input.astype(jnp.float32), vit_ln_gain).astype(jnp.bfloat16)
    w_qkv_flat = w_qkv.reshape(patch_width, 3 * head_cols)
    projected = jnp.dot(
        gather(normed_patches, "tp", 0).reshape(tp_size * own_patches, patch_width),
        w_qkv_flat,
        preferred_element_type=jnp.float32,
    ).astype(jnp.bfloat16)
    group_patches = projected.shape[0]
    projected = projected.reshape(group_patches, 3, local_heads, HD)
    image_index = image_ids(image_lengths[0], group_patches)
    attended = attend(projected[:, 0], projected[:, 1], projected[:, 2], image_index).reshape(
        group_patches, head_cols
    )
    attn_part = jnp.dot(attended, w_proj, preferred_element_type=jnp.float32).astype(jnp.bfloat16)
    attn_sum = scatter_sum(
        attn_part.reshape(tp_size, own_patches, patch_width), "tp", jnp.float32, 1
    )
    vit_out = vit_input.astype(jnp.float32) + attn_sum
    own_tokens = own_patches // 4
    merged_in = (
        layer_norm(vit_out, merger_ln_gain)
        .astype(jnp.bfloat16)
        .reshape(own_tokens, 4 * patch_width)
    )
    expanded = jax.nn.gelu(
        jnp.dot(
            gather(merged_in, "tp", 2).reshape(tp_size * own_tokens, 4 * patch_width),
            merger_w1,
            preferred_element_type=jnp.float32,
        ),
        approximate=False,
    ).astype(jnp.bfloat16)
    vis_part = jnp.dot(expanded, merger_w2, preferred_element_type=jnp.float32).astype(jnp.bfloat16)
    model_width = merger_w2.shape[1]
    vis_rows = scatter_sum(
        vis_part.reshape(tp_size, own_tokens, model_width), "tp", jnp.bfloat16, 3
    )
    seq_size = lax.axis_size("seq")
    slice_width = model_width // seq_size
    vis_values = vis_rows.astype(jnp.float32)
    row_squares = jnp.sum(vis_values * vis_values, axis=1, keepdims=True)
    inverse = lax.rsqrt(row_squares / D + 1e-06)
    high = inverse.astype(jnp.bfloat16).astype(jnp.float32)
    middle = (inverse - high).astype(jnp.bfloat16).astype(jnp.float32)
    lane = lax.broadcasted_iota(jnp.int32, (own_tokens, 128), 1)
    tail = jnp.where(
        lane == 0, high, jnp.where(lane == 1, middle, jnp.where(lane == 2, inverse - high - middle, 0.0))
    ).astype(jnp.bfloat16)
    payload = jnp.stack(
        [
            jnp.concatenate([vis_rows[:, s * slice_width : (s + 1) * slice_width], tail], axis=1)
            for s in range(seq_size)
        ]
    )
    own_slice = exchange(payload, "seq", 4)
    own_slice = own_slice.reshape(seq_size * own_tokens, slice_width + 128)
    seq_rows = tp_size * seq_size * own_tokens
    all_tokens = gather(own_slice, "tp", 5).reshape(seq_rows, slice_width + 128)
    slots = positions.reshape(seq_size, tp_size, own_tokens).transpose(1, 0, 2).reshape(seq_rows)
    row = lax.broadcasted_iota(jnp.int32, (seq_rows, seq_rows), 0)
    pick = (row == slots[None, :]).astype(jnp.bfloat16)
    ordered = jnp.dot(pick, all_tokens, preferred_element_type=jnp.float32)
    token_values = ordered[:, :slice_width]
    inverse_rms = jnp.sum(ordered[:, slice_width : slice_width + 3], axis=1, keepdims=True)
    normed = (token_values * inverse_rms * norm_gain).astype(jnp.bfloat16)
    hidden_width = gate_up_weight.shape[2]
    weight_rows = gate_up_weight.transpose(1, 2, 0).reshape(2 * hidden_width, slice_width)
    chunks = chunk_count(hidden_width)
    gate_up = lax.dot_general(
        weight_rows, normed, (((1,), (1,)), ((), ())), preferred_element_type=jnp.float32
    ).astype(jnp.bfloat16)
    gate_up = gate_up.reshape(2, chunks, hidden_width // chunks, seq_rows).transpose(1, 0, 2, 3)
    hidden = hidden_values(gate_up, "seq", 6).reshape(hidden_width, seq_rows)
    terms = lax.dot_general(
        hidden, down_weight, (((0,), (0,)), ((), ())), preferred_element_type=jnp.float32
    ).astype(jnp.bfloat16)
    out_rows = seq_rows // tp_size
    down_sum = scatter_sum(terms.reshape(tp_size, out_rows, slice_width), "tp", jnp.float32, 7)
    residual = lax.dynamic_slice_in_dim(token_values, lax.axis_index("tp") * out_rows, out_rows, 0)
    return (residual + down_sum).astype(jnp.bfloat16)


def solution(mesh):
    return jax.shard_map(
        local,
        mesh=mesh,
        in_specs=(
            P(("seq", "tp"), None),
            P("seq", None),
            P(),
            P(),
            P(None, None, "tp"),
            P("tp", None),
            P(),
            P(None, "tp"),
            P("tp", None),
            P("seq"),
            P("seq", None, "tp"),
            P("tp", "seq"),
        ),
        out_specs=P("tp", "seq"),
        check_vma=False,
    )
```
